32 devices in a mesh: zero: 4 (over z), tp: 4 (over x, core), shift: 2 (over y).
Axes of the slice: x: 2, y: 2, z: 4, core: 2. Of those that a mesh axis runs over, the one named last changes fastest.
Arguments:
- train_gate: bfloat16 [4096, 8192], P(('shift', 'zero'), 'tp'), parts along dimension 0, may hold values from -0.125 to 0.125
- low_gate: bfloat16 [4096, 32], P(('shift', 'zero')), parts along dimension 0, may hold values from -0.125 to 0.125
- high_gate: bfloat16 [64, 8192], P('shift', 'tp'), parts along dimension 0, may hold values from -1 to 1
- train_up: bfloat16 [4096, 8192], P(('shift', 'zero'), 'tp'), parts along dimension 0, may hold values from -0.125 to 0.125
- low_up: bfloat16 [4096, 32], P(('shift', 'zero')), parts along dimension 0, may hold values from -0.125 to 0.125
- high_up: bfloat16 [64, 8192], P('shift', 'tp'), parts along dimension 0, may hold values from -1 to 1
- norm_train: float32 [4096], P(('shift', 'zero', 'tp')), parts along dimension 0, may hold values from 0.25 to 1.75
- norm_step: float32 [4096], P(('shift', 'zero', 'tp')), parts along dimension 0, may hold values from -0.3 to 0.3
Outputs:
- ready_gate: bfloat16 [16384, 2048], P(('shift', 'tp')), parts along dimension 0
- ready_up: bfloat16 [16384, 2048], P(('shift', 'tp')), parts along dimension 0
- serve_norm: bfloat16 [4096], P('shift'), parts along dimension 0
The draws below stay inside these ranges and needn't reach their ends.
There are 2 independent parts, one for each index of `shift`. The reference program is written for one: setup_inputs(seed, part) draws one part's arguments, and reference() takes and returns one part's arrays. A program takes and returns all parts, laid end to end along the dimension named above; each array names one. Nothing has to cross between parts.
All inputs are finite; a program needn't handle non-finite values.
Results may differ from the reference program's by a relative error of at most 0.001.
Values may be sent and summed in bfloat16 or wider, within the bound.
A program may use at most 64 MiB of HBM per device.

```python
import jax
import jax.numpy as jnp

D_MODEL = 2048
D_INNER = 8192
RANK = 32


def block_levels(own_key, dims, pieces, smallest, top_value):
    loudness = 1.0
    for position, parts in pieces:
        draws = jax.random.uniform(jax.random.fold_in(jax.random.fold_in(own_key, 6), position), (parts,), jnp.float32, smallest / len(pieces), top_value / len(pieces))
        loudness = loudness * jnp.repeat(jnp.exp(draws), dims[position] // parts).reshape((-1,) + (1,) * (len(dims) - 1 - position))
    return loudness


def scatter_about(rng, extent, spread, limit, pieces=(), kind=jnp.bfloat16):
    array = jax.random.normal(rng, extent, jnp.float32) * spread
    if len(pieces) > 0:
        array = block_levels(rng, extent, pieces, -0.22, 0.18) * array
    return jnp.clip(array, min=-limit, max=limit).astype(kind)


def setup_inputs(seed: int = 0, part: int = 0) -> dict:
    arg_keys = jax.random.split(jax.random.key(seed), 9)
    part_keys = jax.random.split(jax.random.fold_in(arg_keys[8], part), 9)
    return {
        "train_gate": scatter_about(part_keys[0], (D_MODEL, D_INNER), D_MODEL ** -0.5, 0.125, ((0, 4), (1, 4))),
        "low_gate": scatter_about(part_keys[1], (D_MODEL, RANK), D_MODEL ** -0.5, 0.125, ((0, 4),)),
        "high_gate": scatter_about(part_keys[2], (RANK, D_INNER), RANK ** -0.5, 1.0, ((1, 4),)),
        "train_up": scatter_about(part_keys[3], (D_MODEL, D_INNER), D_MODEL ** -0.5, 0.125, ((0, 4), (1, 4))),
        "low_up": scatter_about(part_keys[4], (D_MODEL, RANK), D_MODEL ** -0.5, 0.125, ((0, 4),)),
        "high_up": scatter_about(part_keys[5], (RANK, D_INNER), RANK ** -0.5, 1.0, ((1, 4),)),
        "norm_train": jnp.clip(1.0 + 0.15 * jax.random.normal(part_keys[6], (D_MODEL,), jnp.float32), 0.25, 1.75),
        "norm_step": jnp.clip(jax.random.uniform(part_keys[7], (D_MODEL,), jnp.float32, -0.3, 0.3) * block_levels(part_keys[7], (D_MODEL,), ((0, 16),), -0.4, 0.0), -0.3, 0.3),
    }


mix_rate = 0.5


def reference(train_gate, low_gate, high_gate, train_up, low_up, high_up, norm_train, norm_step):
    latest_gate = train_gate.astype(jnp.float32) + mix_rate * jnp.dot(low_gate, high_gate, preferred_element_type=jnp.float32)
    latest_up = train_up.astype(jnp.float32) + mix_rate * jnp.dot(low_up, high_up, preferred_element_type=jnp.float32)
    ready_gate = latest_gate.T.astype(jnp.bfloat16)
    ready_up = latest_up.T.astype(jnp.bfloat16)
    serve_norm = (norm_train + norm_step).astype(jnp.bfloat16)
    return ready_gate, ready_up, serve_norm
```

```python
import functools

import jax
import jax.numpy as jnp
from jax import lax
from jax.experimental import pallas as pl
from jax.experimental.pallas import tpu as pltpu
from jax.sharding import PartitionSpec as P

mix_rate = 0.5
pieces = 2


def merge_kernel(owner, train_ref, low_ref, high_ref, *rest):
    narrow_ref, ready_ref = rest[-2:]
    product = lax.dot_general(
        low_ref[...], high_ref[...], (((0,), (0,)), ((), ())), preferred_element_type=jnp.float32
    )
    narrow = (train_ref[...].astype(jnp.float32) + mix_rate * product).astype(jnp.bfloat16)
    narrow_ref[...] = narrow
    ready_ref[...] = narrow.T


def place_kernel(owner, chunk_ref, held_ref, ready_ref):
    ready_ref[...] = chunk_ref[...].T


def tile_of(width):
    return 512 if width % 512 == 0 else width


def merge(owner, train, low, high, ready, ready_shape, piece):
    rows, columns = train.shape
    width = columns // pieces
    tile = tile_of(width)
    first = piece * (width // tile)
    in_specs = [
        pl.BlockSpec((rows, tile), lambda j, o: (0, first + j)),
        pl.BlockSpec(low.shape, lambda j, o: (0, 0)),
        pl.BlockSpec((high.shape[0], tile), lambda j, o: (0, first + j)),
    ]
    operands = [owner, train, low, high]
    aliases = {}
    if ready is not None:
        in_specs.append(pl.BlockSpec(memory_space=pl.ANY))
        aliases = {len(operands): 1}
        operands.append(ready)
    return pl.pallas_call(
        merge_kernel,
        grid_spec=pltpu.PrefetchScalarGridSpec(
            num_scalar_prefetch=1,
            grid=(width // tile,),
            in_specs=in_specs,
            out_specs=[
                pl.BlockSpec((rows, tile), lambda j, o: (0, j)),
                pl.BlockSpec((tile, rows), lambda j, o: (first + j, o[0])),
            ],
        ),
        out_shape=[
            jax.ShapeDtypeStruct((rows, width), jnp.bfloat16),
            ready_shape,
        ],
        input_output_aliases=aliases,
        cost_estimate=pl.CostEstimate(
            flops=2 * rows * width * low.shape[0], bytes_accessed=6 * rows * width, transcendentals=0
        ),
        name="merge",
    )(*operands)


def place(owner, chunk, ready, piece):
    rows, width = chunk.shape
    tile = tile_of(width)
    first = piece * (width // tile)
    return pl.pallas_call(
        place_kernel,
        grid_spec=pltpu.PrefetchScalarGridSpec(
            num_scalar_prefetch=1,
            grid=(width // tile,),
            in_specs=[
                pl.BlockSpec((rows, tile), lambda j, o: (0, j)),
                pl.BlockSpec(memory_space=pl.ANY),
            ],
            out_specs=pl.BlockSpec((tile, rows), lambda j, o: (first + j, o[0])),
        ),
        out_shape=jax.ShapeDtypeStruct(ready.shape, ready.dtype),
        input_output_aliases={2: 0},
        cost_estimate=pl.CostEstimate(flops=0, bytes_accessed=4 * rows * width, transcendentals=0),
        name="place",
    )(owner, chunk, ready)


def body(n, train_gate, low_gate, high_gate, train_up, low_up, high_up, norm_train, norm_step):
    me = lax.axis_index("zero")
    ring = [(i, (i + 1) % n) for i in range(n)]
    owner = [jnp.reshape(lax.rem(me + (n - step), n), (1,)).astype(jnp.int32) for step in range(n)]
    rows, columns = train_gate.shape
    ready_shape = jax.ShapeDtypeStruct((columns, n * rows), jnp.bfloat16)
    layers = ((train_gate, low_gate.T, high_gate), (train_up, low_up.T, high_up))
    ready = [None] * len(layers)
    flying = {}
    for which, (train, low, high) in enumerate(layers):
        for piece in range(pieces):
            narrow, ready[which] = merge(owner[0], train, low, high, ready[which], ready_shape, piece)
            flying[which, piece] = narrow
    serve_norm = lax.all_gather(
        (norm_train + norm_step).astype(jnp.bfloat16), ("zero", "tp"), axis=0, tiled=True
    )
    for step in range(1, n):
        for which, piece in list(flying):
            flying[which, piece] = lax.ppermute(flying[which, piece], "zero", ring)
            ready[which] = place(owner[step], flying[which, piece], ready[which], piece)
    return ready[0], ready[1], serve_norm


def solution(mesh):
    in_specs = (
        P(("shift", "zero"), "tp"),
        P(("shift", "zero"), None),
        P("shift", "tp"),
        P(("shift", "zero"), "tp"),
        P(("shift", "zero"), None),
        P("shift", "tp"),
        P(("shift", "zero", "tp")),
        P(("shift", "zero", "tp")),
    )
    out_specs = (P(("shift", "tp"), None), P(("shift", "tp"), None), P("shift"))
    return jax.shard_map(
        functools.partial(body, mesh.shape["zero"]),
        mesh=mesh,
        in_specs=in_specs,
        out_specs=out_specs,
        check_vma=False,
    )
```
